32 devices in a mesh: dp: 2 (over x), sp: 4 (over z), tp: 4 (over y, core).
Axes of the slice: x: 2, y: 2, z: 4, core: 2. Of those that a mesh axis runs over, the one named last changes fastest.
Arguments:
- x_in: bfloat16 [256, 3072], P('dp'), parts along dimension 0
- lengths: int32 [256], P('dp'), parts along dimension 0
- w_q: bfloat16 [2, 3072, 3072], P(None, None, 'tp')
- w_k: bfloat16 [2, 3072, 1024], P(None, None, 'tp')
- w_v: bfloat16 [2, 3072, 1024], P(None, None, 'tp')
- w_o: bfloat16 [2, 3072, 3072], P(None, 'tp')
- w_gate: bfloat16 [2, 3072, 8192], P(None, None, 'tp')
- w_up: bfloat16 [2, 3072, 8192], P(None, None, 'tp')
- w_down: bfloat16 [2, 8192, 3072], P(None, 'tp')
- gain_attn: bfloat16 [2, 3072], replicated
- gain_mlp: bfloat16 [2, 3072], replicated
- k_cache: bfloat16 [2, 256, 8, 512, 128], P(None, 'dp', 'tp', 'sp'), parts along dimension 1
- v_cache: bfloat16 [2, 256, 8, 512, 128], P(None, 'dp', 'tp', 'sp'), parts along dimension 1
Outputs:
- output 1: bfloat16 [256, 3072], P('dp'), parts along dimension 0
- output 2: bfloat16 [2, 256, 8, 128], P(None, 'dp', 'tp'), parts along dimension 1
- output 3: bfloat16 [2, 256, 8, 128], P(None, 'dp', 'tp'), parts along dimension 1
There are 2 independent parts. The reference program is written for one: setup_inputs(seed, part) draws one part's arguments, and reference() takes and returns one part's arrays. A program takes and returns all parts, laid end to end along the dimension named above; an argument that names none is the same for every part.
All inputs are finite; a program needn't handle non-finite values.
Results may differ from the reference program's by a relative error of at most 0.02.
Values are sent between devices in bfloat16 or wider.
A program may use at most 1 GiB of HBM per device.

```python
import math
import jax
import jax.numpy as jnp
from jax import lax

D = 3072
HQ = 24
HKV = 8
DH = 128
FF = 8192
LAYERS = 2
BATCH = 128
T_CACHE = 512

GROUP_SIZE = HQ // HKV
LOG_SPAN = int(math.log2(T_CACHE))
EPSILON = 1e-5
NEG_BIG = -1e30


def draw_lengths(len_key):
    key_uni, key_shift, key_base = jax.random.split(len_key, 3)
    uniform_len = jax.random.randint(key_uni, (BATCH,), 1, T_CACHE + 1)
    shift_amt = jax.random.randint(key_shift, (BATCH,), 0, LOG_SPAN + 1)
    short_len = 1 + jnp.right_shift(jax.random.randint(key_base, (BATCH,), 0, T_CACHE), shift_amt)
    seq_idx = jnp.arange(BATCH)
    seq_lens = jnp.where(seq_idx % 4 == 0, T_CACHE, jnp.where(seq_idx % 4 == 1, short_len, uniform_len))
    seq_lens = jnp.where(seq_idx == 1, 1, seq_lens)
    return seq_lens.astype(jnp.int32)


def normal_bf16(rand_key, arr_shape, weight_scale):
    return (jax.random.normal(rand_key, arr_shape, jnp.float32) * weight_scale).astype(jnp.bfloat16)


def setup_inputs(seed: int = 0, part: int = 0) -> dict:
    shared_keys = jax.random.split(jax.random.key(seed), 9)
    part_keys = jax.random.split(jax.random.fold_in(jax.random.key(seed + 1), part), 3)
    len_key = jax.random.fold_in(jax.random.key(seed + 2), part)
    gain_attn = (1.0 + 0.5 * jax.random.normal(shared_keys[7], (LAYERS, D), jnp.float32)).astype(jnp.bfloat16)
    gain_mlp = (1.0 + 0.5 * jax.random.normal(shared_keys[8], (LAYERS, D), jnp.float32)).astype(jnp.bfloat16)
    return {
        "x_in": normal_bf16(part_keys[0], (BATCH, D), 1.0),
        "lengths": draw_lengths(len_key),
        "w_q": normal_bf16(shared_keys[0], (LAYERS, D, HQ * DH), 3.0 * D ** -0.5),
        "w_k": normal_bf16(shared_keys[1], (LAYERS, D, HKV * DH), D ** -0.5),
        "w_v": normal_bf16(shared_keys[2], (LAYERS, D, HKV * DH), D ** -0.5),
        "w_o": normal_bf16(shared_keys[3], (LAYERS, HQ * DH, D), (HQ * DH) ** -0.5),
        "w_gate": normal_bf16(shared_keys[4], (LAYERS, D, FF), D ** -0.5),
        "w_up": normal_bf16(shared_keys[5], (LAYERS, D, FF), D ** -0.5),
        "w_down": normal_bf16(shared_keys[6], (LAYERS, FF, D), 1.5 * FF ** -0.5),
        "gain_attn": gain_attn,
        "gain_mlp": gain_mlp,
        "k_cache": normal_bf16(part_keys[1], (LAYERS, BATCH, HKV, T_CACHE, DH), 1.0),
        "v_cache": normal_bf16(part_keys[2], (LAYERS, BATCH, HKV, T_CACHE, DH), 1.0),
    }


def rms_norm(residual, gain_vec):
    wide_res = residual.astype(jnp.float32)
    mean_sq = jnp.mean(wide_res * wide_res, axis=-1, keepdims=True)
    return (wide_res * lax.rsqrt(mean_sq + EPSILON) * gain_vec.astype(jnp.float32)).astype(jnp.bfloat16)


def reference(x_in, lengths, w_q, w_k, w_v, w_o, w_gate, w_up, w_down, gain_attn, gain_mlp, k_cache, v_cache):
    positions = jnp.arange(T_CACHE)
    score_scale = DH ** -0.5

    def one_sequence(seq_args):
        q_row, k_row, v_row, k_seq, v_seq, seq_len = seq_args
        q_heads = q_row.reshape(HKV, GROUP_SIZE, DH).astype(jnp.float32)
        k_head = k_row.reshape(HKV, DH).astype(jnp.float32)
        v_head = v_row.reshape(HKV, DH).astype(jnp.float32)
        valid_mask = positions < seq_len
        scores = jnp.einsum("kgd,ktd->kgt", q_heads, k_seq.astype(jnp.float32)) * score_scale
        scores = jnp.where(valid_mask, scores, NEG_BIG)
        new_score = jnp.einsum("kgd,kd->kg", q_heads, k_head) * score_scale
        run_max = jnp.maximum(jnp.max(scores, axis=-1), new_score)
        prob_w = jnp.where(valid_mask, jnp.exp(scores - run_max[..., None]), 0.0)
        prob_new = jnp.exp(new_score - run_max)
        denom_sum = jnp.sum(prob_w, axis=-1) + prob_new
        numer_sum = jnp.einsum("kgt,ktd->kgd", prob_w.astype(jnp.bfloat16).astype(jnp.float32), v_seq.astype(jnp.float32))
        numer_sum = numer_sum + prob_new.astype(jnp.bfloat16).astype(jnp.float32)[..., None] * v_head[:, None, :]
        return (numer_sum / denom_sum[..., None]).astype(jnp.bfloat16).reshape(HQ * DH)

    def layer_step(residual, layer_args):
        q_weight, k_weight, v_weight, o_weight, gate_weight, up_weight, down_weight, attn_gain, mlp_gain, k_layer, v_layer = layer_args
        normed = rms_norm(residual, attn_gain)
        query_vec = jnp.dot(normed, q_weight, preferred_element_type=jnp.float32).astype(jnp.bfloat16)
        key_new = jnp.dot(normed, k_weight, preferred_element_type=jnp.float32).astype(jnp.bfloat16)
        val_new = jnp.dot(normed, v_weight, preferred_element_type=jnp.float32).astype(jnp.bfloat16)
        attn_out = lax.map(one_sequence, (query_vec, key_new, val_new, k_layer, v_layer, lengths))
        attn_sum = jnp.dot(attn_out, o_weight, preferred_element_type=jnp.float32)
        residual = (residual.astype(jnp.float32) + attn_sum).astype(jnp.bfloat16)
        normed_mlp = rms_norm(residual, mlp_gain)
        gate_proj = jnp.dot(normed_mlp, gate_weight, preferred_element_type=jnp.float32)
        up_proj = jnp.dot(normed_mlp, up_weight, preferred_element_type=jnp.float32)
        hidden_act = (jax.nn.silu(gate_proj) * up_proj).astype(jnp.bfloat16)
        mlp_sum = jnp.dot(hidden_act, down_weight, preferred_element_type=jnp.float32)
        residual = (residual.astype(jnp.float32) + mlp_sum).astype(jnp.bfloat16)
        return residual, (key_new.reshape(BATCH, HKV, DH), val_new.reshape(BATCH, HKV, DH))

    x_out, new_kv = lax.scan(layer_step, x_in, (w_q, w_k, w_v, w_o, w_gate, w_up, w_down, gain_attn, gain_mlp, k_cache, v_cache))
    return x_out, new_kv[0], new_kv[1]
```

```python
import functools

import jax
import jax.numpy as jnp
from jax import lax
from jax.experimental import pallas as pl
from jax.experimental.pallas import tpu as pltpu
from jax.sharding import PartitionSpec as P

MESH = pl.DeviceIdType.MESH
EPSILON = 1e-5
NEG_BIG = -1e30
BF = jnp.bfloat16
F32 = jnp.float32


def dot(a, b):
    return jnp.dot(a, b, preferred_element_type=F32)


def dot_t(a, b):
    return lax.dot_general(a, b, (((1,), (1,)), ((), ())), preferred_element_type=F32)


def kernel(cfg, lens, x_hbm, wq, wk, wv, wo, wg, wu, wd, ga, gm, kc, vc, x_out, k_out, v_out, *scratch):
    (gu, kb, vb, wob, wdb, xbuf, hbuf, acc, qown, qrecv, qs, os, oown, osend, orecv, stsend, strecv, attn, act,
     msend, mrecv, ysend, yrecv, s_qkv, s_kv, s_w, s_gu, q_s, q_r, kv_s, kv_r, o_s, o_r, st_s, st_r,
     m_s, m_r, y_s, y_r, x_s, x_r, f_s, f_r, g_s, g_r) = scratch
    n_layers, n_sp, rows, d_model, q_cols, kv_cols, ff, dh = cfg
    n_q = q_cols // dh
    n_kv = kv_cols // dh
    group = n_q // n_kv
    t_loc = kb.shape[1] // rows // n_kv
    z = lax.axis_index("sp")
    t = lax.axis_index("tp")
    core = lax.rem(t, 2)
    mate = t + 1 - 2 * core
    ypeer = lax.rem(t + 2, 4)
    half = d_model // 2
    n_ch = 2
    ch_w = half // n_ch
    k_ch = 4
    k_w = d_model // k_ch
    scale = dh ** -0.5
    order = (0, 1, 3, 2)

    def up(d):
        return lax.rem(z + d, n_sp)

    def down(d):
        return lax.rem(z + n_sp - d, n_sp)

    def row_ds(src):
        return pl.ds(pl.multiple_of(src * rows, rows), rows)

    def rcopy(src, dst, ss, rs, **dev):
        return pltpu.make_async_remote_copy(src_ref=src, dst_ref=dst, send_sem=ss, recv_sem=rs, device_id=dev, device_id_type=MESH)

    def qkv_copies(l):
        out = []
        for c in range(k_ch):
            r = pl.ds(c * k_w, k_w)
            out.append((
                pltpu.make_async_copy(wq.at[l, r, :], gu.at[r, pl.ds(0, q_cols)], s_qkv.at[c, 0]),
                pltpu.make_async_copy(wk.at[l, r, :], gu.at[r, pl.ds(q_cols, kv_cols)], s_qkv.at[c, 1]),
                pltpu.make_async_copy(wv.at[l, r, :], gu.at[r, pl.ds(q_cols + kv_cols, kv_cols)], s_qkv.at[c, 2]),
            ))
        return out

    def kv_copies(l, j):
        src = pl.multiple_of(down(order[j]) * kb.shape[1], kb.shape[1])
        r = pl.ds(src, kb.shape[1])
        return (pltpu.make_async_copy(kc.at[l, r, :], kb.at[j], s_kv.at[j, 0]),
                pltpu.make_async_copy(vc.at[l, r, :], vb.at[j], s_kv.at[j, 1]))

    def gu_copies(l):
        return (pltpu.make_async_copy(wg.at[l], gu.at[:, pl.ds(0, ff)], s_gu.at[0]),
                pltpu.make_async_copy(wu.at[l], gu.at[:, pl.ds(ff, ff)], s_gu.at[1]))

    def wo_copy(l):
        return pltpu.make_async_copy(wo.at[l], wob, s_w.at[0])

    def wd_copy(l):
        return pltpu.make_async_copy(wd.at[l], wdb, s_w.at[1])

    x_copy = pltpu.make_async_copy(x_hbm.at[row_ds(z), :], xbuf.at[0], s_w.at[2])

    def start_qkv(l):
        for c in qkv_copies(l):
            for cp in c:
                cp.start()

    def start_kv(l):
        for j in range(n_sp):
            for cp in kv_copies(l, j):
                cp.start()

    x_copy.start()
    start_qkv(0)
    start_kv(0)
    wo_copy(0).start()

    barrier = pltpu.get_barrier_semaphore()
    for d in range(1, n_sp):
        pl.semaphore_signal(barrier, inc=1, device_id={"sp": up(d)}, device_id_type=MESH)
    pl.semaphore_signal(barrier, inc=1, device_id={"tp": mate}, device_id_type=MESH)
    pl.semaphore_signal(barrier, inc=1, device_id={"tp": ypeer}, device_id_type=MESH)

    qs[...] = jnp.zeros_like(qs)
    row_i = lax.broadcasted_iota(jnp.int32, (8, dh), 0)
    lane_i = lax.broadcasted_iota(jnp.int32, (8, dh), 1)
    lane_r = lax.broadcasted_iota(jnp.int32, (rows, dh), 1)
    first_kv = row_i < group

    pending = []
    reuse = ([], [])

    def send(cp):
        cp.start()
        pending.append(cp)

    def norm(src_ref, gain_row):
        w = 512
        tot = jnp.zeros((rows, 128), F32)
        for c in range(d_model // 128):
            xw = src_ref[:, c * 128:(c + 1) * 128].astype(F32)
            tot = tot + xw * xw
        inv = lax.rsqrt(jnp.sum(tot, axis=-1, keepdims=True) / d_model + EPSILON)
        for c in range(d_model // w):
            cols = slice(c * w, (c + 1) * w)
            hbuf[:, cols] = (src_ref[:, cols].astype(F32) * inv * gain_row[:, cols].astype(F32)).astype(BF)

    def attend(l, j):
        src = down(order[j])
        base = src * rows
        for cp in kv_copies(l, j):
            cp.wait()
        unroll = 8

        def body(i, carry):
            st_m, st_s = carry
            ps = []
            for u in range(unroll):
                b = i * unroll + u
                q = qs[pl.ds(pl.multiple_of(b * 8, 8), 8), :].astype(BF)
                k = kb[j, pl.ds(pl.multiple_of(b * n_kv * t_loc, n_kv * t_loc), n_kv * t_loc), :]
                s2 = dot_t(q, k)
                s = jnp.where(first_kv, s2[:, :t_loc], s2[:, t_loc:]) * scale
                mask = (z * t_loc + lane_i) < lens[base + b]
                s = jnp.where(mask, s, NEG_BIG)
                m = jnp.max(s, axis=1, keepdims=True)
                p = jnp.where(mask, jnp.exp(s - m), 0.0)
                tot = jnp.sum(p, axis=1, keepdims=True)
                st_m = jnp.where(lane_i == b, m, st_m)
                st_s = jnp.where(lane_i == b, tot, st_s)
                ps.append(jnp.concatenate([jnp.where(first_kv, p, 0.0), jnp.where(first_kv, 0.0, p)], axis=1).astype(BF))
            for u in range(unroll):
                b = i * unroll + u
                v = vb[j, pl.ds(pl.multiple_of(b * n_kv * t_loc, n_kv * t_loc), n_kv * t_loc), :]
                os[pl.ds(pl.multiple_of(b * 8, 8), 8), :] = dot(ps[u], v)
            return st_m, st_s

        zero = jnp.zeros((8, dh), F32)
        st_m, st_s = lax.fori_loop(0, rows // unroll, body, (zero, zero))
        return jnp.concatenate([st_m, st_s, jnp.zeros((dh - 16, dh), F32)], axis=0).T[:rows, :]

    def reduce(stage, lhs, w_ref, last):
        def part(col):
            return dot(lhs[...], w_ref[:, pl.ds(pl.multiple_of(col, 128), ch_w)])

        m_cp, y_cp = [], []
        par = stage % 2
        for cp in reuse[par]:
            cp.wait_send()
        reuse[par].clear()
        for c in range(n_ch):
            msend[par, c] = part((1 - core) * half + c * ch_w).astype(BF)
            cp = rcopy(msend.at[par, c], mrecv.at[par, c], m_s.at[stage, c], m_r.at[stage, c], tp=mate)
            cp.start()
            reuse[par].append(cp)
            m_cp.append(cp)
        for c in range(n_ch):
            p = part(core * half + c * ch_w)
            m_cp[c].wait_recv()
            ysend[par, c] = (p + mrecv[par, c].astype(F32)).astype(BF)
            cp = rcopy(ysend.at[par, c], yrecv.at[par, c], y_s.at[stage, c], y_r.at[stage, c], tp=ypeer)
            cp.start()
            reuse[par].append(cp)
            y_cp.append(cp)
        x_cp = []
        for c in range(n_ch):
            cols = pl.ds(pl.multiple_of(core * half + c * ch_w, 128), ch_w)
            y_cp[c].wait_recv()
            tot = ysend[par, c].astype(F32) + yrecv[par, c].astype(F32)
            new = (xbuf[stage, :, cols].astype(F32) + tot).astype(BF)
            if last:
                dst = x_out.at[row_ds(z), cols]
            else:
                dst = xbuf.at[stage + 1, :, cols]
            dst[...] = new
            cp = rcopy(dst, dst, x_s.at[stage, c], x_r.at[stage, c], tp=mate)
            send(cp)
            x_cp.append(cp)
            if last:
                for d in (2, 1, 3):
                    send(rcopy(dst, dst, f_s.at[d - 1, c], f_r.at[d - 1, c], sp=up(d)))
        if last:
            for d in (1, 3, 2):
                for c in range(n_ch):
                    cols = pl.ds(pl.multiple_of(core * half + c * ch_w, 128), ch_w)
                    dst = x_out.at[row_ds(down(d)), cols]
                    rcopy(dst, dst, f_s.at[d - 1, c], f_r.at[d - 1, c], sp=up(d)).wait_recv()
                    send(rcopy(dst, dst, g_s.at[d - 1, c], g_r.at[d - 1, c], tp=mate))
        for cp in x_cp:
            cp.wait_recv()
        if last:
            for d in (1, 3, 2):
                for c in range(n_ch):
                    cols = pl.ds(pl.multiple_of((1 - core) * half + c * ch_w, 128), ch_w)
                    dst = x_out.at[row_ds(down(d)), cols]
                    rcopy(dst, dst, g_s.at[d - 1, c], g_r.at[d - 1, c], tp=mate).wait_recv()

    for l in range(n_layers):
        if l == 0:
            x_copy.wait()
        norm(xbuf.at[2 * l], ga[l:l + 1, :])
        for c, cps in enumerate(qkv_copies(l)):
            for cp in cps:
                cp.wait()
            r = pl.ds(c * k_w, k_w)
            val = dot(hbuf[:, r], gu[r, pl.ds(0, q_cols + 2 * kv_cols)])
            if c == 0:
                acc[...] = val
            else:
                acc[...] += val
        for cp in gu_copies(l):
            cp.start()
        if l == 0:
            wd_copy(0).start()
        if l == 0:
            pl.semaphore_wait(barrier, n_sp - 1 + 2)
        for h in range(n_q):
            qown[l, h] = acc[:, h * dh:(h + 1) * dh].astype(BF)
        q_cp = {}
        for d in (2, 1, 3):
            q_cp[d] = rcopy(qown.at[l], qrecv.at[l, d - 1], q_s.at[l, d - 1], q_r.at[l, d - 1], sp=up(d))
            send(q_cp[d])
        own = row_ds(z)
        k_out[l, own, :] = acc[:, q_cols:q_cols + kv_cols].astype(BF)
        v_out[l, own, :] = acc[:, q_cols + kv_cols:].astype(BF)
        kv_cp = []
        for d in (2, 1, 3):
            for i, ref in enumerate((k_out, v_out)):
                cp = rcopy(ref.at[l, own, :], ref.at[l, own, :], kv_s.at[l, d - 1, i], kv_r.at[l, d - 1, i], sp=up(d))
                send(cp)
                kv_cp.append((d, i, ref))

        o_cp = {}
        stats_own = None
        for j in range(n_sp):
            d = order[j]
            q_src = qown.at[l] if d == 0 else qrecv.at[l, d - 1]
            if d:
                q_cp[d].wait_recv()
            for h in range(n_q):
                qs[pl.ds(h, rows, stride=8), :] = q_src[h].astype(F32)
            st = attend(l, j)
            if d == 0:
                stats_own = st
                for h in range(n_q):
                    oown[h] = os[pl.ds(h, rows, stride=8), :]
            else:
                for h in range(n_q):
                    osend[l, d - 1, h] = os[pl.ds(h, rows, stride=8), :].astype(BF)
                stsend[l, d - 1] = st
                a = rcopy(osend.at[l, d - 1], orecv.at[l, d - 1], o_s.at[l, d - 1], o_r.at[l, d - 1], sp=down(d))
                b = rcopy(stsend.at[l, d - 1], strecv.at[l, d - 1], st_s.at[l, d - 1], st_r.at[l, d - 1], sp=down(d))
                send(b)
                send(a)
                o_cp[d] = (a, b)
        if l + 1 < n_layers:
            start_kv(l + 1)

        new_s = jnp.zeros((rows, dh), F32)
        for h in range(n_q):
            g = h // group
            qh = qown[l, h].astype(F32)
            kh = k_out[l, own, g * dh:(g + 1) * dh].astype(F32)
            new_s = jnp.where(lane_r == h, jnp.sum(qh * kh, axis=1, keepdims=True) * scale, new_s)
        for d in range(1, n_sp):
            o_cp[d][1].wait_recv()
        stats = [stats_own] + [strecv[l, d - 1] for d in range(1, n_sp)]
        top = new_s
        for st in stats:
            top = jnp.maximum(top, st)
        p_new = jnp.exp(new_s - top)
        wts = [jnp.exp(st - top) for st in stats]
        denom = p_new
        for st, w in zip(stats, wts):
            denom = denom + w * pltpu.roll(st, dh - 8, 1)
        wts = [w / denom for w in wts]
        w_new = p_new.astype(BF).astype(F32) / denom
        for d in range(1, n_sp):
            o_cp[d][0].wait_recv()
        for h in range(n_q):
            g = h // group
            o = wts[0][:, h:h + 1] * oown[h]
            for d in range(1, n_sp):
                o = o + wts[d][:, h:h + 1] * orecv[l, d - 1, h].astype(F32)
            o = o + w_new[:, h:h + 1] * v_out[l, own, g * dh:(g + 1) * dh].astype(F32)
            attn[:, h * dh:(h + 1) * dh] = o.astype(BF)

        wo_copy(l).wait()
        reduce(2 * l, attn, wob, False)
        if l + 1 < n_layers:
            wo_copy(l + 1).start()
        norm(xbuf.at[2 * l + 1], gm[l:l + 1, :])
        for cp in gu_copies(l):
            cp.wait()
        f_w = 256

        def mlp_body(i, carry):
            c0 = pl.multiple_of(i * f_w, f_w)
            gate = dot(hbuf[...], gu[:, pl.ds(c0, f_w)])
            upv = dot(hbuf[...], gu[:, pl.ds(pl.multiple_of(ff + i * f_w, f_w), f_w)])
            act[:, pl.ds(c0, f_w)] = (gate * jax.nn.sigmoid(gate) * upv).astype(BF)
            return carry

        lax.fori_loop(0, ff // f_w, mlp_body, 0)
        if l + 1 < n_layers:
            start_qkv(l + 1)
        wd_copy(l).wait()
        reduce(2 * l + 1, act, wdb, l == n_layers - 1)
        if l + 1 < n_layers:
            wd_copy(l + 1).start()
        for d, i, ref in kv_cp:
            dst = ref.at[l, row_ds(down(d)), :]
            rcopy(dst, dst, kv_s.at[l, d - 1, i], kv_r.at[l, d - 1, i], sp=up(d)).wait_recv()

    for cp in pending + reuse[0] + reuse[1]:
        cp.wait_send()


def solution(mesh):
    n_sp = mesh.shape["sp"]
    weight_col = P(None, None, "tp")
    weight_row = P(None, "tp", None)
    cache_spec = P(None, "dp", "tp", "sp", None)
    new_spec = P(None, "dp", "tp", None)

    def device_step(x_in, lengths, w_q, w_k, w_v, w_o, w_gate, w_up, w_down, gain_attn, gain_mlp, k_cache, v_cache):
        n_l, batch, n_kv, t_loc, dh = k_cache.shape
        d_model = x_in.shape[1]
        rows = batch // n_sp
        q_cols, kv_cols, ff = w_q.shape[2], w_k.shape[2], w_gate.shape[2]
        n_q = q_cols // dh
        kc = k_cache.reshape(n_l, batch * n_kv * t_loc, dh)
        vc = v_cache.reshape(n_l, batch * n_kv * t_loc, dh)
        cfg = (n_l, n_sp, rows, d_model, q_cols, kv_cols, ff, dh)
        stages = 2 * n_l
        half = d_model // 2
        dma = pltpu.SemaphoreType.DMA
        any_spec = pl.BlockSpec(memory_space=pl.ANY)
        vmem = pl.BlockSpec(memory_space=pltpu.VMEM)
        o3 = n_sp - 1
        scratch = [
            pltpu.VMEM((d_model, 2 * ff), BF),
            pltpu.VMEM((n_sp, rows * n_kv * t_loc, dh), BF),
            pltpu.VMEM((n_sp, rows * n_kv * t_loc, dh), BF),
            pltpu.VMEM((q_cols, d_model), BF),
            pltpu.VMEM((ff, d_model), BF),
            pltpu.VMEM((stages, rows, d_model), BF),
            pltpu.VMEM((rows, d_model), BF),
            pltpu.VMEM((rows, q_cols + 2 * kv_cols), F32),
            pltpu.VMEM((n_l, n_q, rows, dh), BF),
            pltpu.VMEM((n_l, o3, n_q, rows, dh), BF),
            pltpu.VMEM((rows * 8, dh), F32),
            pltpu.VMEM((rows * 8, dh), F32),
            pltpu.VMEM((n_q, rows, dh), F32),
            pltpu.VMEM((n_l, o3, n_q, rows, dh), BF),
            pltpu.VMEM((n_l, o3, n_q, rows, dh), BF),
            pltpu.VMEM((n_l, o3, rows, dh), F32),
            pltpu.VMEM((n_l, o3, rows, dh), F32),
            pltpu.VMEM((rows, q_cols), BF),
            pltpu.VMEM((rows, ff), BF),
        ] + [pltpu.VMEM((2, 2, rows, half // 2), BF)] * 4 + [
            dma((4, 3)), dma((n_sp, 2)), dma((3,)), dma((2,)),
            dma((n_l, o3)), dma((n_l, o3)), dma((n_l, o3, 2)), dma((n_l, o3, 2)),
            dma((n_l, o3)), dma((n_l, o3)), dma((n_l, o3)), dma((n_l, o3)),
            dma((stages, 2)), dma((stages, 2)), dma((stages, 2)), dma((stages, 2)), dma((stages, 2)), dma((stages, 2)),
            dma((o3, 2)), dma((o3, 2)), dma((o3, 2)), dma((o3, 2)),
        ]
        x_out, k_new, v_new = pl.pallas_call(
            functools.partial(kernel, cfg),
            out_shape=(
                jax.ShapeDtypeStruct((batch, d_model), BF),
                jax.ShapeDtypeStruct((n_l, batch, kv_cols), BF),
                jax.ShapeDtypeStruct((n_l, batch, kv_cols), BF),
            ),
            in_specs=[pl.BlockSpec(memory_space=pltpu.SMEM)] + [any_spec] * 8 + [vmem, vmem] + [any_spec] * 2,
            out_specs=(vmem, vmem, vmem),
            scratch_shapes=scratch,
            compiler_params=pltpu.CompilerParams(collective_id=0, has_side_effects=True, vmem_limit_bytes=67043328),
        )(lengths, x_in, w_q, w_k, w_v, w_o, w_gate, w_up, w_down, gain_attn, gain_mlp, kc, vc)
        return x_out, k_new.reshape(n_l, batch, n_kv, dh), v_new.reshape(n_l, batch, n_kv, dh)

    in_specs = (P("dp", None), P("dp"), weight_col, weight_col, weight_col, weight_row, weight_col, weight_col, weight_row, P(None, None), P(None, None), cache_spec, cache_spec)
    out_specs = (P("dp", None), new_spec, new_spec)
    return jax.shard_map(device_step, mesh=mesh, in_specs=in_specs, out_specs=out_specs, check_vma=False)
```
